32 devices in a mesh: row: 8 (over z, x), col: 4 (over y, core).
Axes of the slice: x: 2, y: 2, z: 4, core: 2. Of those that a mesh axis runs over, the one named last changes fastest.
Arguments:
- matrix: float32 [16384, 16384], P('row', 'col'), may hold values from -300 to 300, as said below
Outputs:
- trailing: float32 [16384, 16384], P('row', 'col')
- reflectors: float32 [16384, 8], P('row')
The draws below stay inside these ranges and needn't reach their ends.
Inputs may be any that keep to these rules, and one draw needn't show every extreme that they name: matrix is exactly symmetric.
All inputs are finite; a program needn't handle non-finite values.
Results may differ from the reference program's by a relative error of at most 0.00021.
Values sent between devices are 32-bit elements; how exact they have to be, the bound alone decides.
A program may use at most 128 MiB of HBM per device.

```python
import math
import jax
import jax.numpy as jnp
from jax import lax

N = 16384
COLS = 8


def draw_matrix(key, part):
    first_key, second_key = jax.random.split(jax.random.fold_in(key, 11))
    positions = jnp.arange(N, dtype=jnp.float32)
    rising = jnp.exp(0.5 * math.log(3.0) * positions / N)
    entries = jnp.clip(jax.random.normal(first_key, (N, N), jnp.float32), -6.0, 6.0)
    spread = jnp.exp(0.5 * jax.random.uniform(second_key, (N,), jnp.float32, 0.0, math.log(10.0)))
    symmetric = (entries + entries.T) * (1.0 / math.sqrt(2.0))
    scales = rising * spread
    outer = scales[:, None] * scales[None, :]
    return (symmetric * outer).astype(jnp.float32)


def setup_inputs(seed: int = 0) -> dict:
    streams_of = jax.random.split(jax.random.key(seed), 2)
    return {
        "matrix": draw_matrix(jax.random.fold_in(streams_of[1], 71), 0),
    }


def precise_dot(operand, factor):
    return jnp.dot(operand, factor, precision=lax.Precision.HIGHEST, preferred_element_type=jnp.float32)

def reference(matrix):
    reflect = jnp.zeros((N, COLS), jnp.float32)
    companion = jnp.zeros((N, COLS), jnp.float32)
    positions = jnp.arange(N, dtype=jnp.int32)
    for column in range(COLS):
        current = matrix[:, column] - precise_dot(reflect, companion[column]) - precise_dot(companion, reflect[column])
        below_part = jnp.where(positions > column, current, 0.0)
        squared = jnp.sum(below_part * below_part)
        leading = jnp.sum(jnp.where(positions == column + 1, current, 0.0))
        length = jnp.sqrt(squared)
        vector = below_part + jnp.where(positions == column + 1, length, 0.0)
        scaling = 1.0 / (length * (length + leading))
        column_image = precise_dot(matrix, vector)
        weight_comp = precise_dot(companion.T, vector)
        weight_refl = precise_dot(reflect.T, vector)
        pushed = scaling * (column_image - precise_dot(reflect, weight_comp) - precise_dot(companion, weight_refl))
        inner_product = jnp.sum(pushed * vector)
        update = pushed - 0.5 * scaling * inner_product * vector
        reflect = reflect.at[:, column].set(vector)
        companion = companion.at[:, column].set(update)
    trailing = matrix - precise_dot(reflect, companion.T) - precise_dot(companion, reflect.T)
    return (trailing, reflect)
```

```python
import functools

import jax
import jax.numpy as jnp
from jax import lax
from jax.experimental import pallas as pl
from jax.experimental.pallas import tpu as pltpu
from jax.sharding import PartitionSpec as P

COLS = 8
LANES = 128
GUARD = 4.0
MESH = pl.DeviceIdType.MESH

def from_root(block, axis, source):
    block = jnp.where(lax.axis_index(axis) == source, block, jnp.zeros_like(block))
    return lax.psum(block, axis)


def precise_dot(operand, factor):
    return jnp.dot(
        operand, factor, precision=lax.Precision.HIGHEST, preferred_element_type=jnp.float32
    )


def local_general(matrix):
    rows_local = matrix.shape[0]
    cols_local = matrix.shape[1]
    row_index = lax.axis_index("row")
    col_index = lax.axis_index("col")
    panel = from_root(matrix[:, :COLS], "col", 0)
    whole_panel = lax.all_gather(panel, "row", axis=0, tiled=True)
    all_ids = jnp.arange(whole_panel.shape[0], dtype=jnp.int32)
    reflect = jnp.zeros((all_ids.shape[0], COLS), jnp.float32)
    companion = jnp.zeros((all_ids.shape[0], COLS), jnp.float32)
    for column in range(COLS):
        reflect_rows = lax.dynamic_slice_in_dim(reflect, row_index * rows_local, rows_local, 0)
        companion_rows = lax.dynamic_slice_in_dim(companion, row_index * rows_local, rows_local, 0)
        current = (
            whole_panel[:, column]
            - precise_dot(reflect, companion[column])
            - precise_dot(companion, reflect[column])
        )
        below_whole = jnp.where(all_ids > column, current, 0.0)
        squared = jnp.sum(below_whole * below_whole)
        leading = jnp.sum(jnp.where(all_ids == column + 1, current, 0.0))
        length = jnp.sqrt(squared)
        vector = below_whole + jnp.where(all_ids == column + 1, length, 0.0)
        scaling = 1.0 / (length * (length + leading))
        vector_rows = lax.dynamic_slice_in_dim(vector, row_index * rows_local, rows_local, 0)
        vector_cols = lax.dynamic_slice_in_dim(vector, col_index * cols_local, cols_local, 0)
        weight_comp = precise_dot(companion.T, vector)
        weight_refl = precise_dot(reflect.T, vector)
        row_image = lax.psum(precise_dot(matrix, vector_cols), "col")
        pushed = scaling * (
            row_image
            - precise_dot(reflect_rows, weight_comp)
            - precise_dot(companion_rows, weight_refl)
        )
        inner_product = lax.psum(jnp.sum(pushed * vector_rows), "row")
        update_rows = pushed - 0.5 * scaling * inner_product * vector_rows
        update = lax.all_gather(update_rows, "row", axis=0, tiled=True)
        reflect = reflect.at[:, column].set(vector)
        companion = companion.at[:, column].set(update)
    reflect_rows = lax.dynamic_slice_in_dim(reflect, row_index * rows_local, rows_local, 0)
    companion_rows = lax.dynamic_slice_in_dim(companion, row_index * rows_local, rows_local, 0)
    reflect_cols = lax.dynamic_slice_in_dim(reflect, col_index * cols_local, cols_local, 0)
    companion_cols = lax.dynamic_slice_in_dim(companion, col_index * cols_local, cols_local, 0)
    trailing = (
        matrix
        - precise_dot(reflect_rows, companion_cols.T)
        - precise_dot(companion_rows, reflect_cols.T)
    )
    return (trailing, reflect_rows)


def total(values):
    folded = jnp.sum(values, axis=0)
    return jnp.sum(jnp.sum(folded, axis=0, keepdims=True), axis=1, keepdims=True)


def pick(values, chosen):
    kept = jnp.where(chosen, values, 0.0)
    return jnp.sum(jnp.sum(kept, axis=0, keepdims=True), axis=1, keepdims=True)


def plain_kernel(
    nr, nc, a_hbm, left_ref, right_ref, a,
    raw, mine, panel, acc, part, arrived, image, vecs, comps, nxt, corr,
    load_sem, scatter_sem, raw_sem, psend_sem, precv_sem,
    send1_sem, recv1_sem, send2_sem, recv2_sem,
):
    r = lax.axis_index("row")
    c = lax.axis_index("col")
    n = nr * nc
    rows, cols = a.shape
    quarter = rows // nc
    width = cols // nr
    subs = quarter // LANES
    tiles = cols // LANES
    here = r * nc + c

    def flip(t):
        return t + 1 - 2 * lax.rem(t, 2)

    def turn(i):
        t = lax.rem(c + 2 * (nc // 2 - 1 - i // 2), nc)
        own = i >= nc - 2
        second = lax.rem(i, 2) == 1
        first_of = jnp.where(own, flip(c), t)
        second_of = jnp.where(own, c, flip(t))
        return jnp.where(second, second_of, first_of)

    def load(i):
        at = pl.ds(pl.multiple_of(turn(i) * quarter, quarter), quarter)
        return pltpu.make_async_copy(a_hbm.at[at], a.at[at], load_sem.at[i])

    def rowcopy(q):
        at = pl.ds(pl.multiple_of(q * width, width), width)
        return a_hbm.at[pl.ds(0, COLS), at]

    @pl.when(r == 0)
    def _():
        pltpu.make_async_copy(rowcopy(0), raw, raw_sem).start()

    for i in range(nc):
        load(i).start()

    barrier = pltpu.get_barrier_semaphore()

    def greet(d, carry):
        t = lax.rem(here + d, n)
        pl.semaphore_signal(barrier, inc=1, device_id=(t // nc, lax.rem(t, nc)), device_id_type=MESH)
        return carry

    lax.fori_loop(1, n, greet, 0)

    def clear(k, carry):
        vecs[k] = jnp.zeros(vecs.shape[1:], jnp.float32)
        comps[k] = jnp.zeros(comps.shape[1:], jnp.float32)
        return carry

    lax.fori_loop(0, COLS + 1, clear, 0)
    pl.semaphore_wait(barrier, n - 1)

    def scatter(q):
        return pltpu.make_async_remote_copy(
            src_ref=rowcopy(q), dst_ref=raw, send_sem=scatter_sem.at[q], recv_sem=raw_sem,
            device_id=(q, c), device_id_type=MESH,
        )

    @pl.when(r == 0)
    def _():
        for q in range(1, nr):
            scatter(q).start()

    pltpu.make_async_copy(raw, raw, raw_sem).wait()
    for k in range(COLS):
        for m in range(subs):
            mine[k, m : m + 1, :] = raw[k : k + 1, m * LANES : (m + 1) * LANES]
    spot = c * nr + r
    panel[spot] = mine[...]

    def spread(d, carry):
        t = lax.rem(here + d, n)
        pltpu.make_async_remote_copy(
            src_ref=mine, dst_ref=panel.at[spot], send_sem=psend_sem, recv_sem=precv_sem,
            device_id=(t // nc, lax.rem(t, nc)), device_id_type=MESH,
        ).start()
        return carry

    lax.fori_loop(1, n, spread, 0)
    most = panel.at[pl.ds(0, n - 1)]
    pltpu.make_async_copy(most, most, precv_sem).wait()
    pltpu.make_async_copy(most, most, psend_sem).wait()

    @pl.when(r == 0)
    def _():
        for q in range(1, nr):
            scatter(q).wait_send()

    ids = lax.broadcasted_iota(jnp.int32, (subs, LANES), 0) * LANES + lax.broadcasted_iota(
        jnp.int32, (subs, LANES), 1
    )

    def reflect(column, current):
        vecs[column] = current
        head = jnp.where(ids > column, current[0], 0.0)
        vecs[column, 0] = head
        below = vecs[column]
        squared = total(below * below)
        leading = pick(head, ids == column + 1)
        length = jnp.sqrt(squared)
        vecs[column, 0] = head + jnp.where(ids == column + 1, length, 0.0)
        return 1.0 / (length * (length + leading))

    def step(j, scaling):
        vrows = [
            jnp.broadcast_to(vecs[j, c * nr + t // subs, t % subs : t % subs + 1, :], (8, LANES))
            for t in range(tiles)
        ]

        def block(i, carry):
            k = turn(i)

            @pl.when(j == 0)
            def _():
                load(i).wait()

            def group(g, inner):
                at = pl.ds(pl.multiple_of(k * quarter + g * 8, 8), 8)
                sums = [None] * 4
                for t in range(tiles):
                    term = a[at, t * LANES : (t + 1) * LANES] * vrows[t]
                    sums[t % 4] = term if sums[t % 4] is None else sums[t % 4] + term
                acc[pl.ds(pl.multiple_of(g * 8, 8), 8), :] = (sums[0] + sums[1]) + (sums[2] + sums[3])
                return inner

            lax.fori_loop(0, quarter // 8, group, 0, unroll=16)
            for m in range(subs):
                turned = acc[m * LANES : (m + 1) * LANES, :].T
                part[k, m : m + 1, :] = jnp.sum(turned, axis=0, keepdims=True)

            @pl.when(i < nc - 1)
            def _():
                first(k).start()

            return carry

        def first(k):
            return pltpu.make_async_remote_copy(
                src_ref=part.at[k], dst_ref=arrived.at[c], send_sem=send1_sem.at[k],
                recv_sem=recv1_sem.at[c], device_id=(r, k), device_id_type=MESH,
            )

        lax.fori_loop(0, nc, block, 0)
        value = part[c]

        def collect(d, value):
            k = lax.rem(c + d, nc)
            pltpu.make_async_copy(arrived.at[k], arrived.at[k], recv1_sem.at[k]).wait()
            return value + arrived[k]

        value = lax.fori_loop(1, nc, collect, value, unroll=True)
        image[j, here] = value

        def second(d, carry):
            t = lax.rem(here + d, n)
            pltpu.make_async_remote_copy(
                src_ref=image.at[j, here], dst_ref=image.at[j, here], send_sem=send2_sem,
                recv_sem=recv2_sem.at[j], device_id=(t // nc, lax.rem(t, nc)), device_id_type=MESH,
            ).start()
            return carry

        for d in sorted(range(1, n), key=lambda d: abs(d - n // 2)):
            second(d, 0)

        vector = vecs[j]
        corr[...] = jnp.zeros(corr.shape, jnp.float32)
        follow = jnp.minimum(j + 1, COLS - 1)
        nxt[...] = panel[:, follow]
        target = ids == j + 1

        def history(k, carry):
            v_k = vecs[k]
            w_k = comps[k]
            corr[...] = corr[...] + v_k * total(w_k * vecs[j]) + w_k * total(v_k * vecs[j])
            nxt[...] = nxt[...] - v_k * pick(w_k[0], target) - w_k * pick(v_k[0], target)
            return carry

        lax.fori_loop(0, j, history, 0)

        def sent(d, carry):
            k = lax.rem(c + d, nc)
            pltpu.make_async_copy(part.at[k], part.at[k], send1_sem.at[k]).wait()
            return carry

        lax.fori_loop(1, nc, sent, 0)
        rest = image.at[j, pl.ds(0, n - 1)]
        pltpu.make_async_copy(rest, rest, send2_sem).wait()
        pltpu.make_async_copy(rest, rest, recv2_sem.at[j]).wait()

        pushed = scaling * (image[j] - corr[...])
        inner_product = total(pushed * vector)
        update = pushed - (0.5 * scaling * inner_product) * vector
        comps[j] = update
        current = nxt[...] - vector * pick(update[0], target) - update * pick(vector[0], target)
        return reflect(j + 1, current)

    lax.fori_loop(0, COLS, step, reflect(0, panel[:, 0]))

    def place(dest, base, count):
        def move(p, carry):
            for m in range(subs):
                at = pl.ds(pl.multiple_of((p * subs + m) * LANES, LANES), LANES)
                for k in range(COLS):
                    dest[k : k + 1, at] = vecs[k, base + p, m : m + 1, :]
                    dest[COLS + k : COLS + k + 1, at] = comps[k, base + p, m : m + 1, :]
            return carry

        lax.fori_loop(0, count, move, 0)

    place(left_ref, r * nc, nc)
    place(right_ref, c * nr, nr)
    left_ref[2 * COLS :, :] = jnp.zeros((COLS, rows), jnp.float32)


def plain_call(nr, nc, matrix):
    rows, cols = matrix.shape
    n = nr * nc
    subs = rows // nc // LANES
    vector = (n, subs, LANES)
    f32 = jnp.float32
    vmem = pl.BlockSpec(memory_space=pltpu.VMEM)
    dma = pltpu.SemaphoreType.DMA
    return pl.pallas_call(
        functools.partial(plain_kernel, nr, nc),
        out_shape=(
            jax.ShapeDtypeStruct((3 * COLS, rows), f32),
            jax.ShapeDtypeStruct((2 * COLS, cols), f32),
            pltpu.VMEM((rows, cols), f32),
        ),
        in_specs=[pl.BlockSpec(memory_space=pl.ANY)],
        out_specs=(vmem, vmem, vmem),
        scratch_shapes=[
            pltpu.VMEM((COLS, cols // nr), f32),
            pltpu.VMEM((COLS, subs, LANES), f32),
            pltpu.VMEM((n, COLS, subs, LANES), f32),
            pltpu.VMEM((rows // nc, LANES), f32),
            pltpu.VMEM((nc, subs, LANES), f32),
            pltpu.VMEM((nc, subs, LANES), f32),
            pltpu.VMEM((COLS,) + vector, f32),
            pltpu.VMEM((COLS + 1,) + vector, f32),
            pltpu.VMEM((COLS + 1,) + vector, f32),
            pltpu.VMEM(vector, f32),
            pltpu.VMEM(vector, f32),
            dma((nc,)), dma((nr,)), dma, dma, dma,
            dma((nc,)), dma((nc,)), dma, dma((COLS,)),
        ],
        compiler_params=pltpu.CompilerParams(
            collective_id=1, has_side_effects=True, vmem_limit_bytes=8 * 1024 * 1024
        ),
    )(matrix)


def lane_sum(values):
    return jnp.broadcast_to(jnp.sum(values, axis=1, keepdims=True), values.shape)


def row_sum(values):
    return jnp.sum(values, axis=0, keepdims=True)


def panel_kernel(
    nr, nc, a_hbm, left_ref, right_ref, a,
    lanes, acc, pan_r, pan_c, pan_h, head_out,
    v_r, w_r, y_r, m_r, p_r, q_r, z_r, base_r,
    v_c, w_c, y_c, m_c, p_c, q_c, z_c, base_c,
    v_h, w_h, g_old, h_old, g_new, h_new, wj_next, vj_next, keep, dots,
    part_c, part_r, note_r, note_c,
    load_sem, strip_sem, pan_send, pan_recv, cross_send, pan_cross, head_send, head_recv,
    part_send, part_recv, back_send, back_recv, far_send, far_recv,
    rows_send, rows_recv, note_send, note_r_recv, note_c_recv,
):
    r = lax.axis_index("row")
    c = lax.axis_index("col")
    n = nr * nc
    here = r * nc + c
    rows, cols = a.shape
    deep = rows // LANES
    wide = cols // LANES
    chunks = wide // 8
    width = cols // chunks
    half = deep // 2
    group = nr // (nc // 2)
    side = lax.rem(c, 2)
    owner = r // 2
    f32 = jnp.float32

    def load(q):
        return pltpu.make_async_copy(
            a_hbm.at[:, pl.ds(q * width, width)], a.at[:, pl.ds(q * width, width)], load_sem.at[q]
        )

    strip = pltpu.make_async_copy(a_hbm.at[:, pl.ds(0, LANES)], lanes, strip_sem)

    @pl.when(c == 0)
    def _():
        strip.start()

    @pl.when(c != 0)
    def _():
        for q in range(chunks):
            load(q).start()

    barrier = pltpu.get_barrier_semaphore()

    def greet(d, carry):
        t = lax.rem(here + d, n)
        pl.semaphore_signal(barrier, inc=1, device_id=(t // nc, lax.rem(t, nc)), device_id_type=MESH)
        return carry

    lax.fori_loop(1, n, greet, 0)

    for ref in (v_r, w_r, v_c, w_c, v_h, w_h, g_old, h_old, keep, dots, p_r, p_c):
        ref[...] = jnp.zeros(ref.shape, f32)
    y_r[0] = jnp.zeros(y_r.shape[1:], f32)
    y_c[0] = jnp.zeros(y_c.shape[1:], f32)

    def to(src, dst, send, recv, row, col):
        return pltpu.make_async_remote_copy(
            src_ref=src, dst_ref=dst, send_sem=send, recv_sem=recv,
            device_id=(row, col), device_id_type=MESH,
        )

    def drain(ref, sem):
        pltpu.make_async_copy(ref, ref, sem).wait()

    used = pl.ds(0, COLS + 1)
    first = pl.ds(0, 1)
    others = pl.ds(1, COLS)

    @pl.when(c == 0)
    def _():
        strip.wait()
        for q in range(chunks):
            load(q).start()

        def turn(b, carry):
            turned = lanes[pl.ds(pl.multiple_of(b * LANES, LANES), LANES), :].T
            for k in range(COLS + 1):
                pan_r[k, pl.ds(b, 1), :] = turned[k : k + 1, :]
            return carry

        lax.fori_loop(0, deep, turn, 0)

    pl.semaphore_wait(barrier, n - 1)

    @pl.when(c == 0)
    def _():
        for d in range(1, nc):
            to(pan_r.at[first], pan_r.at[first], pan_send.at[d - 1], pan_recv.at[0], r, d).start()
        for d in range(1, nc):
            to(pan_r.at[others], pan_r.at[others], pan_send.at[nc + d - 1], pan_recv.at[1], r, d).start()

    @pl.when(c != 0)
    def _():
        drain(pan_r.at[first], pan_recv.at[0])

    def spread(source, target, width_of, send, recv):
        for i in range(group):
            row = (c // 2) * group + i
            mine = jnp.logical_and(row == r, c == owner)

            @pl.when(jnp.logical_not(mine))
            def _(i=i, row=row):
                to(source(side), target(lax.rem(r, 2), side), send.at[i], recv.at[2 * lax.rem(r, 2) + side], row, owner).start()

    def collect(target, recv):
        for kind in range(2):
            for part in range(2):
                mine = jnp.logical_and(r == 2 * c + kind, c == part + 2 * (r // group))

                @pl.when(jnp.logical_not(mine))
                def _(kind=kind, part=part):
                    drain(target(kind, part), recv.at[2 * kind + part])

    def spread_done(source, send):
        for i in range(group):
            row = (c // 2) * group + i
            mine = jnp.logical_and(row == r, c == owner)

            @pl.when(jnp.logical_not(mine))
            def _(i=i):
                drain(source(side), send.at[i])

    def keeps_own():
        return jnp.logical_and(c == owner, r // group == c // 2)

    def piece(part):
        return pl.ds(pl.multiple_of(part * half, half), half)

    def spot(kind, part):
        return pl.ds(pl.multiple_of(kind * deep + part * half, half), half)

    def pan_source(part):
        return pan_r.at[used, piece(part)]

    def pan_target(kind, part):
        return pan_c.at[used, spot(kind, part)]

    def share_panel():
        @pl.when(c != 0)
        def _():
            drain(pan_r.at[others], pan_recv.at[1])

        spread(pan_source, pan_target, None, cross_send, pan_cross)

        @pl.when(keeps_own())
        def _():
            pan_c[used, spot(lax.rem(r, 2), side)] = pan_r[used, piece(side)]

        @pl.when(r == 0)
        def _():
            for k in range(COLS + 1):
                head_out[k : k + 1, :] = pan_r[k, 0:1, :]
                pan_h[k : k + 1, :] = pan_r[k, 0:1, :]
            for d in range(1, nr):
                to(head_out, pan_h, head_send.at[d - 1], head_recv, d, c).start()

    ids_r = (
        r * rows
        + lax.broadcasted_iota(jnp.int32, (deep, LANES), 0) * LANES
        + lax.broadcasted_iota(jnp.int32, (deep, LANES), 1)
    )
    ids_c = (
        c * cols
        + lax.broadcasted_iota(jnp.int32, (wide, LANES), 0) * LANES
        + lax.broadcasted_iota(jnp.int32, (wide, LANES), 1)
    )
    lane1 = lax.broadcasted_iota(jnp.int32, (1, LANES), 1)
    lane8 = lax.broadcasted_iota(jnp.int32, (8, LANES), 1)
    row8 = lax.broadcasted_iota(jnp.int32, (8, LANES), 0)
    lane24 = lax.broadcasted_iota(jnp.int32, (24, LANES), 1)
    row24 = lax.broadcasted_iota(jnp.int32, (24, LANES), 0)

    dom_r = (pan_r, v_r, w_r, y_r, m_r, p_r, q_r, z_r, base_r, ids_r)
    dom_c = (pan_c, v_c, w_c, y_c, m_c, p_c, q_c, z_c, base_c, ids_c)

    m_r[...] = jnp.where(ids_r > 0, pan_r[0], 0.0)

    def send_notes(j, dom, note, slot, me, count, peer):
        _, v, w, y, m, p, _, _, _, ids = dom
        jm = jnp.maximum(j - 1, 0)
        operand = m[...]
        push = p[...]
        last = v[jm]
        for k in range(COLS):
            dots[k : k + 1, :] = row_sum(w[k] * operand)
            dots[COLS + k : COLS + k + 1, :] = row_sum(v[k] * operand)
        cut = jnp.where(ids > j, last, 0.0)
        dots[16:17, :] = row_sum(push * operand)
        dots[17:18, :] = row_sum(push * last)
        dots[18:19, :] = row_sum(operand * operand)
        dots[19:20, :] = row_sum(operand * cut)
        dots[20:21, :] = row_sum(cut * cut)
        sums = lane_sum(dots[...])
        note[slot, me, 0:1, :] = row_sum(jnp.where(lane24 == row24, sums, 0.0))
        note[slot, me, 1:2, :] = y[j, 0:1, :]
        recv = note_r_recv if count == nr else note_c_recv
        for d in range(1, count):
            row, col = peer(d)
            to(note.at[slot, me], note.at[slot, me], note_send, recv.at[slot], row, col).start()

    def take_notes(note, slot, count):
        recv = note_r_recv if count == nr else note_c_recv
        drain(note.at[slot, pl.ds(0, count - 1)], recv.at[slot])
        drain(note.at[slot, pl.ds(0, count - 1)], note_send)
        total = note[slot, 0, 0:1, :]
        for k in range(1, count):
            total = total + note[slot, k, 0:1, :]
        spread24 = jnp.broadcast_to(total, (24, LANES))
        return lane_sum(jnp.where(lane24 == row24, spread24, 0.0)), note[slot, 0, 1:2, :]

    def settle(j, dom, out, sums, y_head):
        jm = jnp.maximum(j - 1, 0)
        jrow = pl.ds(jm, 1)
        s_old = keep[0:1, :]
        bad = keep[1:2, :]
        pm, pv, mm, mv, vv = (sums[16 + i : 17 + i, :] for i in range(5))
        alpha = 0.5 * s_old * pv
        gold = g_old[...]
        hold = h_old[...]
        vh = v_h[...]
        pan, v, w, y, m, p, _, _, _, ids = out
        old = y[j]
        s1 = jnp.zeros(old.shape, f32)
        for k in range(COLS):
            s1 = s1 + v[k] * gold[k : k + 1, :] + w[k] * hold[k : k + 1, :]
        p_head = s_old * (y_head - row_sum(vh * gold + w_h[...] * hold))
        v_head = v_h[jrow, :]
        w_h[jrow, :] = p_head - alpha * v_head
        wh = w_h[...]
        now8 = lane8 == j
        next8 = lane8 == j + 1
        vj = lane_sum(jnp.where(now8, vh, 0.0))
        wj = lane_sum(jnp.where(now8, wh, 0.0))
        vn = lane_sum(jnp.where(next8, vh, 0.0))
        wn = lane_sum(jnp.where(next8, wh, 0.0))
        v_at = lane_sum(jnp.where(lane1 == j, v_head, 0.0))
        p_at = lane_sum(jnp.where(lane1 == j, p_head, 0.0))
        coef = 2.0 * alpha * v_at - p_at
        before = row8 < j - 1
        vjb = jnp.where(before, vj, 0.0)
        wjb = jnp.where(before, wj, 0.0)
        x_head = pan_h[pl.ds(j, 1), :] - row_sum(vh * wjb + wh * vjb) - p_head * v_at
        b_head = jnp.where(lane1 > j, x_head + coef * v_head, 0.0)
        lead = lane_sum(jnp.where(lane1 == j + 1, b_head, 0.0))
        squared = mm + 2.0 * coef * mv + coef * coef * vv
        length = jnp.sqrt(squared)
        v_h[pl.ds(j, 1), :] = b_head + jnp.where(lane1 == j + 1, length, 0.0)
        scale = 1.0 / (length * (length + lead))
        pivot = lead + length
        kappa = scale * pivot
        fine = (mm + coef * coef * vv) <= GUARD * squared
        keep[0:1, :] = scale
        keep[1:2, :] = jnp.where(fine, bad, 1.0)
        keep[2:3, :] = kappa
        at_last = row8 == jm
        v_sq = vv + v_at * v_at
        gold = gold + jnp.where(at_last, pv - alpha * v_sq, 0.0)
        hold = hold + jnp.where(at_last, v_sq, 0.0)
        gn = sums[0:8, :] + jnp.where(at_last, pm - alpha * mv, 0.0) + coef * (gold - wj * v_at) + length * wn
        hn = sums[8:16, :] + coef * (hold - vj * v_at) + length * vn
        live = row8 < j
        gn = jnp.where(live, gn, 0.0)
        hn = jnp.where(live, hn, 0.0)
        g_old[...] = gn
        h_old[...] = hn

        _, vd, wd, _, md, pd, _, _, _, ids_d = dom
        last_d = vd[jm]
        wd[jm] = pd[...] - alpha * last_d
        vd[j] = (
            md[...] + coef * jnp.where(ids_d > j, last_d, 0.0) + jnp.where(ids_d == j + 1, length, 0.0)
        )

        last = v[jm]
        push = s_old * (old - s1)
        w[jm] = push - alpha * last
        s2 = jnp.zeros(old.shape, f32)
        s3 = jnp.zeros(old.shape, f32)
        s4 = jnp.zeros(old.shape, f32)
        for k in range(COLS):
            v_k = v[k]
            w_k = w[k]
            s2 = s2 + v_k * wjb[k : k + 1, :] + w_k * vjb[k : k + 1, :]
            s3 = s3 + v_k * gn[k : k + 1, :] + w_k * hn[k : k + 1, :]
            s4 = s4 + v_k * wn[k : k + 1, :] + w_k * vn[k : k + 1, :]
        a_now = pan[j]
        a_next = pan[j + 1]
        x = a_now - s2 - push * v_at
        b = jnp.where(ids > j, x + coef * last, 0.0)
        v[j] = b + jnp.where(ids == j + 1, length, 0.0)
        extra = coef * (old - v_at * a_now) + length * a_next
        out[6][...] = extra
        base = extra - s3
        out[8][...] = base
        out[7][...] = a_next - s4 - kappa * base

    def absorb(j, out, at, value):
        _, _, _, y, m, p, extra, z, base, ids = out
        scale = keep[0:1, :]
        kappa = keep[2:3, :]
        y[j + 1, at, :] = value + extra[at, :]
        p[at, :] = scale * (value + base[at, :])
        return z[at, :] - kappa * value

    blocks = rows // LANES
    batch = 4
    groups = LANES // 8

    def tile(row, t):
        return a[pl.ds(pl.multiple_of(row, 8), 8), t * LANES : (t + 1) * LANES]

    def turn_rows(b):
        for k in range(batch):
            at = pl.ds(pl.multiple_of((b * batch + k) * LANES, LANES), LANES)
            lanes[at, :] = jnp.broadcast_to(m_r[pl.ds(b * batch + k, 1), :], (LANES, LANES)).T

    def down(q):
        many = batch if q == 0 else 1

        def block(b, sums):
            factors = [
                lanes[pl.ds(pl.multiple_of(b * many * LANES + g * 8, 8), 8), :]
                for g in range(many * groups)
            ]
            if q == 0:
                turn_rows(jnp.minimum(b + 1, blocks // batch - 1))
            for g in range(many * groups):
                row = b * many * LANES + g * 8
                sums = tuple(
                    sums[t] + tile(row, q * 8 + t) * factors[g] for t in range(8)
                )
            return sums

        if q == 0:
            turn_rows(0)
        return lax.fori_loop(0, blocks // many, block, tuple(jnp.zeros((8, LANES), f32) for _ in range(8)))

    def across(q, slot):
        factors = [jnp.broadcast_to(m_c[q * 8 + t : q * 8 + t + 1, :], (8, LANES)) for t in range(8)]
        final = q == chunks - 1
        many = batch if final else 1

        def fold(b):
            for k in range(batch):
                turned = acc[pl.ds(pl.multiple_of((b * batch + k) * LANES, LANES), LANES), :].T
                part_r[slot, c, pl.ds(b * batch + k, 1), :] = row_sum(turned)

        def block(b, carry):
            if final:
                fold(jnp.maximum(b - 1, 0))
            for g in range(many * groups):
                row = b * many * LANES + g * 8
                at = pl.ds(pl.multiple_of(row, 8), 8)
                terms = [tile(row, q * 8 + t) * factors[t] for t in range(8)]
                while len(terms) > 1:
                    terms = [terms[i] + terms[i + 1] for i in range(0, len(terms), 2)]
                acc[at, :] = terms[0] if q == 0 else acc[at, :] + terms[0]
            return carry

        lax.fori_loop(0, blocks // many, block, 0)
        if final:
            fold(blocks // batch - 1)

    def in_rows(d):
        return lax.rem(r + d, nr), c

    def in_cols(d):
        return r, lax.rem(c + d, nc)

    def back_source(j):
        return y_c.at[j + 1, pl.ds(pl.multiple_of(lax.rem(r, 2) * deep, deep), deep)]

    def pair(i, carry):
        j = 2 * i
        send_notes(j, dom_r, note_r, i, r, nr, in_rows)
        for q in range(chunks):
            @pl.when(i == 0)
            def _(q=q):
                load(q).wait()
                if q == 1:
                    share_panel()

            sums = down(q)
            for t in range(8):
                part_c[i, q, r, t : t + 1, :] = row_sum(sums[t])
            for d in range(1, nr):
                row, col = in_rows(d)
                mine = part_c.at[i, q, r]
                to(mine, mine, part_send, part_recv.at[i, q], row, col).start()

        @pl.when(i == 0)
        def _():
            collect(pan_target, pan_cross)

            @pl.when(r != 0)
            def _():
                drain(pan_h, head_recv)

        @pl.when(i > 0)
        def _():
            collect(lambda kind, part: y_c.at[j, spot(kind, part)], far_recv.at[i])
            spread_done(lambda part: y_r.at[j, piece(part)], far_send)
            drain(part_r.at[i, pl.ds(0, nc - 1)], rows_send)

        sums, y_head = take_notes(note_r, i, nr)
        settle(j, dom_r, dom_c, sums, y_head)

        for q in range(chunks):
            drain(part_c.at[i, q, pl.ds(0, nr - 1)], part_recv.at[i, q])
            value = part_c[i, q, 0]
            for k in range(1, nr):
                value = value + part_c[i, q, k]
            at = pl.ds(q * 8, 8)
            m_c[at, :] = jnp.where(ids_c[q * 8 : q * 8 + 8, :] > j + 1, absorb(j, dom_c, at, value), 0.0)
            if q == chunks - 1:
                @pl.when(c == owner)
                def _():
                    for d in range(1, nc):
                        to(back_source(j), y_r.at[j + 1], back_send.at[d - 1], back_recv.at[i], r, lax.rem(c + d, nc)).start()
                    y_r[j + 1] = y_c[j + 1, pl.ds(pl.multiple_of(lax.rem(r, 2) * deep, deep), deep)]

                send_notes(j + 1, dom_c, note_c, i, c, nc, in_cols)
            across(q, i)

        mine = part_r.at[i, c]
        for d in range(1, nc):
            row, col = in_cols(d)
            to(mine, mine, rows_send, rows_recv.at[i], row, col).start()
        drain(part_c.at[i, :, pl.ds(0, nr - 1)], part_send)

        @pl.when(c != owner)
        def _():
            drain(y_r.at[j + 1], back_recv.at[i])

        @pl.when(c == owner)
        def _():
            for d in range(1, nc):
                drain(back_source(j), back_send.at[d - 1])

        sums, y_head = take_notes(note_c, i, nc)
        settle(j + 1, dom_c, dom_r, sums, y_head)
        drain(part_r.at[i, pl.ds(0, nc - 1)], rows_recv.at[i])
        value = part_r[i, 0]
        for k in range(1, nc):
            value = value + part_r[i, k]
        m_r[...] = jnp.where(ids_r > j + 2, absorb(j + 1, dom_r, slice(None), value), 0.0)

        def far_source(part):
            return y_r.at[j + 2, piece(part)]

        spread(far_source, lambda kind, part: y_c.at[j + 2, spot(kind, part)], None, far_send, far_recv.at[i + 1])

        @pl.when(keeps_own())
        def _():
            y_c[j + 2, spot(lax.rem(r, 2), side)] = y_r[j + 2, piece(side)]

        return carry

    lax.fori_loop(0, COLS // 2, pair, 0)

    last = COLS // 2
    send_notes(COLS, dom_r, note_r, last, r, nr, in_rows)

    @pl.when(c == 0)
    def _():
        for d in range(1, nc):
            drain(pan_r.at[first], pan_send.at[d - 1])
            drain(pan_r.at[others], pan_send.at[nc + d - 1])

    spread_done(pan_source, cross_send)

    @pl.when(r == 0)
    def _():
        for d in range(1, nr):
            drain(head_out, head_send.at[d - 1])

    def place(dest, values, base, blocks_of):
        for b in range(blocks_of):
            for k in range(COLS):
                dest[base + k : base + k + 1, b * LANES : (b + 1) * LANES] = values[k, b : b + 1, :]

    place(left_ref, v_r, 0, deep)
    place(right_ref, v_c, 0, wide)
    collect(lambda kind, part: y_c.at[COLS, spot(kind, part)], far_recv.at[last])
    spread_done(lambda part: y_r.at[COLS, piece(part)], far_send)
    drain(part_r.at[0, pl.ds(0, nc - 1)], rows_send)
    sums, _ = take_notes(note_r, last, nr)
    scale = keep[0:1, :]
    alpha = 0.5 * scale * sums[17:18, :]
    w_r[COLS - 1] = p_r[...] - alpha * v_r[COLS - 1]
    s1 = jnp.zeros((wide, LANES), f32)
    for k in range(COLS - 1):
        s1 = s1 + v_c[k] * g_old[k : k + 1, :] + w_c[k] * h_old[k : k + 1, :]
    w_c[COLS - 1] = scale * (y_c[COLS] - s1) - alpha * v_c[COLS - 1]
    place(left_ref, w_r, COLS, deep)
    place(right_ref, w_c, COLS, wide)
    left_ref[2 * COLS :, :] = jnp.broadcast_to(keep[1:2, 0:1], (COLS, rows))


def panel_call(nr, nc, matrix):
    rows, cols = matrix.shape
    deep, wide = rows // LANES, cols // LANES
    chunks = wide // 8
    f32 = jnp.float32
    vmem = pl.BlockSpec(memory_space=pltpu.VMEM)
    dma = pltpu.SemaphoreType.DMA
    steps = COLS // 2

    def mem(*shape):
        return pltpu.VMEM(shape, f32)

    def domain(size):
        return [
            mem(COLS + 1, size, LANES), mem(COLS + 1, size, LANES), mem(COLS + 1, size, LANES),
            *(mem(size, LANES) for _ in range(5)),
        ]

    return pl.pallas_call(
        functools.partial(panel_kernel, nr, nc),
        out_shape=(
            jax.ShapeDtypeStruct((3 * COLS, rows), f32),
            jax.ShapeDtypeStruct((2 * COLS, cols), f32),
            pltpu.VMEM((rows, cols), f32),
        ),
        in_specs=[pl.BlockSpec(memory_space=pl.ANY)],
        out_specs=(vmem, vmem, vmem),
        scratch_shapes=[
            mem(rows, LANES), mem(rows, LANES),
            mem(COLS + 1, deep, LANES), mem(COLS + 1, wide, LANES), mem(16, LANES), mem(16, LANES),
            *domain(deep), *domain(wide),
            mem(8, LANES), mem(8, LANES), mem(8, LANES), mem(8, LANES), mem(8, LANES), mem(8, LANES),
            mem(8, LANES), mem(8, LANES), mem(8, LANES), mem(24, LANES),
            mem(steps, chunks, nr, 8, LANES), mem(steps, nc, deep, LANES),
            mem(steps + 1, nr, 2, LANES), mem(steps, nc, 2, LANES),
            dma((chunks,)), dma, dma((2 * nc,)), dma((2,)), dma((nr,)), dma((4,)), dma((nr,)), dma,
            dma, dma((steps, chunks)), dma((nc,)), dma((steps,)), dma((nr,)), dma((steps + 1, 4)),
            dma, dma((steps,)), dma, dma((steps + 1,)), dma((steps,)),
        ],
        compiler_params=pltpu.CompilerParams(
            collective_id=0, has_side_effects=True, vmem_limit_bytes=8 * 1024 * 1024
        ),
    )(matrix)


def thirds(values):
    high = values.astype(jnp.bfloat16)
    rest = values - high.astype(jnp.float32)
    middle = rest.astype(jnp.bfloat16)
    low = (rest - middle.astype(jnp.float32)).astype(jnp.bfloat16)
    return high, middle, low


def trailing_kernel(left_ref, right_ref, a_ref, out_ref, refl_ref, flag_ref, stacked):
    @pl.when(pl.program_id(0) == 0)
    def _():
        swapped = jnp.concatenate([right_ref[COLS:, :], right_ref[:COLS, :]], axis=0)
        h, m, l = thirds(swapped)
        stacked[...] = jnp.concatenate([h, m, h, m, l, h], axis=0)

    left = left_ref[: 2 * COLS, :]
    flag_ref[...] = left_ref[2 * COLS :, :LANES]
    h, m, l = thirds(left)
    other = jnp.concatenate([h, h, m, m, h, l], axis=0)
    product = lax.dot_general(
        other, stacked[...], (((0,), (0,)), ((), ())), preferred_element_type=jnp.float32
    )
    at = pl.ds(pl.multiple_of(pl.program_id(0) * out_ref.shape[0], out_ref.shape[0]), out_ref.shape[0])
    out_ref[...] = a_ref[at, :] - product
    refl_ref[...] = left[:COLS, :]


def trailing_call(left, right, matrix):
    rows, cols = matrix.shape
    tile = 128
    return pl.pallas_call(
        trailing_kernel,
        grid=(rows // tile,),
        out_shape=(
            jax.ShapeDtypeStruct((rows, cols), jnp.float32),
            jax.ShapeDtypeStruct((COLS, rows), jnp.float32),
            jax.ShapeDtypeStruct((COLS, LANES), jnp.float32),
        ),
        in_specs=[
            pl.BlockSpec((3 * COLS, tile), lambda i: (0, i)),
            pl.BlockSpec((2 * COLS, cols), lambda i: (0, 0)),
            pl.BlockSpec(memory_space=pltpu.VMEM),
        ],
        out_specs=(
            pl.BlockSpec((tile, cols), lambda i: (i, 0)),
            pl.BlockSpec((COLS, tile), lambda i: (0, i)),
            pl.BlockSpec((COLS, LANES), lambda i: (0, 0)),
        ),
        scratch_shapes=[pltpu.VMEM((12 * COLS, cols), jnp.bfloat16)],
        compiler_params=pltpu.CompilerParams(
            dimension_semantics=("arbitrary",), vmem_limit_bytes=16 * 1024 * 1024
        ),
    )(left, right, matrix)


def local(nr, nc, matrix):
    rows, cols = matrix.shape
    piece = rows // nc
    if rows % (16 * LANES) or cols != 2 * rows or nr != 2 * nc or nc % 2 or piece > 8 * LANES:
        return local_general(matrix)
    left, right, kept = panel_call(nr, nc, matrix)
    trailing, reflectors, flag = trailing_call(left, right, kept)

    def again(state):
        own, _ = lax.optimization_barrier((matrix, state[2]))
        return trailing_call(*plain_call(nr, nc, own))

    trailing, reflectors, _ = lax.while_loop(
        lambda state: jnp.any(state[2] != 0.0), again, (trailing, reflectors, flag)
    )
    return trailing, reflectors.T


def solution(mesh):
    return jax.shard_map(
        functools.partial(local, mesh.shape["row"], mesh.shape["col"]),
        mesh=mesh,
        in_specs=(P("row", "col"),),
        out_specs=(P("row", "col"), P("row", None)),
        check_vma=False,
    )
```

```python
import functools

import jax
import jax.numpy as jnp
from jax import lax
from jax.experimental import pallas as pl
from jax.experimental.pallas import tpu as pltpu
from jax.sharding import PartitionSpec as P

COLS = 8
LANES = 128
GUARD = 4.0
MESH = pl.DeviceIdType.MESH

def from_root(block, axis, source):
    block = jnp.where(lax.axis_index(axis) == source, block, jnp.zeros_like(block))
    return lax.psum(block, axis)


def precise_dot(operand, factor):
    return jnp.dot(
        operand, factor, precision=lax.Precision.HIGHEST, preferred_element_type=jnp.float32
    )


def local_general(matrix):
    rows_local = matrix.shape[0]
    cols_local = matrix.shape[1]
    row_index = lax.axis_index("row")
    col_index = lax.axis_index("col")
    panel = from_root(matrix[:, :COLS], "col", 0)
    whole_panel = lax.all_gather(panel, "row", axis=0, tiled=True)
    all_ids = jnp.arange(whole_panel.shape[0], dtype=jnp.int32)
    reflect = jnp.zeros((all_ids.shape[0], COLS), jnp.float32)
    companion = jnp.zeros((all_ids.shape[0], COLS), jnp.float32)
    for column in range(COLS):
        reflect_rows = lax.dynamic_slice_in_dim(reflect, row_index * rows_local, rows_local, 0)
        companion_rows = lax.dynamic_slice_in_dim(companion, row_index * rows_local, rows_local, 0)
        current = (
            whole_panel[:, column]
            - precise_dot(reflect, companion[column])
            - precise_dot(companion, reflect[column])
        )
        below_whole = jnp.where(all_ids > column, current, 0.0)
        squared = jnp.sum(below_whole * below_whole)
        leading = jnp.sum(jnp.where(all_ids == column + 1, current, 0.0))
        length = jnp.sqrt(squared)
        vector = below_whole + jnp.where(all_ids == column + 1, length, 0.0)
        scaling = 1.0 / (length * (length + leading))
        vector_rows = lax.dynamic_slice_in_dim(vector, row_index * rows_local, rows_local, 0)
        vector_cols = lax.dynamic_slice_in_dim(vector, col_index * cols_local, cols_local, 0)
        weight_comp = precise_dot(companion.T, vector)
        weight_refl = precise_dot(reflect.T, vector)
        row_image = lax.psum(precise_dot(matrix, vector_cols), "col")
        pushed = scaling * (
            row_image
            - precise_dot(reflect_rows, weight_comp)
            - precise_dot(companion_rows, weight_refl)
        )
        inner_product = lax.psum(jnp.sum(pushed * vector_rows), "row")
        update_rows = pushed - 0.5 * scaling * inner_product * vector_rows
        update = lax.all_gather(update_rows, "row", axis=0, tiled=True)
        reflect = reflect.at[:, column].set(vector)
        companion = companion.at[:, column].set(update)
    reflect_rows = lax.dynamic_slice_in_dim(reflect, row_index * rows_local, rows_local, 0)
    companion_rows = lax.dynamic_slice_in_dim(companion, row_index * rows_local, rows_local, 0)
    reflect_cols = lax.dynamic_slice_in_dim(reflect, col_index * cols_local, cols_local, 0)
    companion_cols = lax.dynamic_slice_in_dim(companion, col_index * cols_local, cols_local, 0)
    trailing = (
        matrix
        - precise_dot(reflect_rows, companion_cols.T)
        - precise_dot(companion_rows, reflect_cols.T)
    )
    return (trailing, reflect_rows)


def total(values):
    folded = jnp.sum(values, axis=0)
    return jnp.sum(jnp.sum(folded, axis=0, keepdims=True), axis=1, keepdims=True)


def pick(values, chosen):
    kept = jnp.where(chosen, values, 0.0)
    return jnp.sum(jnp.sum(kept, axis=0, keepdims=True), axis=1, keepdims=True)


def plain_kernel(
    nr, nc, a_hbm, left_ref, right_ref, a,
    raw, mine, panel, acc, part, arrived, image, vecs, comps, nxt, corr,
    load_sem, scatter_sem, raw_sem, psend_sem, precv_sem,
    send1_sem, recv1_sem, send2_sem, recv2_sem,
):
    r = lax.axis_index("row")
    c = lax.axis_index("col")
    n = nr * nc
    rows, cols = a.shape
    quarter = rows // nc
    width = cols // nr
    subs = quarter // LANES
    tiles = cols // LANES
    here = r * nc + c

    def flip(t):
        return t + 1 - 2 * lax.rem(t, 2)

    def turn(i):
        t = lax.rem(c + 2 * (nc // 2 - 1 - i // 2), nc)
        own = i >= nc - 2
        second = lax.rem(i, 2) == 1
        first_of = jnp.where(own, flip(c), t)
        second_of = jnp.where(own, c, flip(t))
        return jnp.where(second, second_of, first_of)

    def load(i):
        at = pl.ds(pl.multiple_of(turn(i) * quarter, quarter), quarter)
        return pltpu.make_async_copy(a_hbm.at[at], a.at[at], load_sem.at[i])

    def rowcopy(q):
        at = pl.ds(pl.multiple_of(q * width, width), width)
        return a_hbm.at[pl.ds(0, COLS), at]

    @pl.when(r == 0)
    def _():
        pltpu.make_async_copy(rowcopy(0), raw, raw_sem).start()

    for i in range(nc):
        load(i).start()

    barrier = pltpu.get_barrier_semaphore()

    def greet(d, carry):
        t = lax.rem(here + d, n)
        pl.semaphore_signal(barrier, inc=1, device_id=(t // nc, lax.rem(t, nc)), device_id_type=MESH)
        return carry

    lax.fori_loop(1, n, greet, 0)

    def clear(k, carry):
        vecs[k] = jnp.zeros(vecs.shape[1:], jnp.float32)
        comps[k] = jnp.zeros(comps.shape[1:], jnp.float32)
        return carry

    lax.fori_loop(0, COLS + 1, clear, 0)
    pl.semaphore_wait(barrier, n - 1)

    def scatter(q):
        return pltpu.make_async_remote_copy(
            src_ref=rowcopy(q), dst_ref=raw, send_sem=scatter_sem.at[q], recv_sem=raw_sem,
            device_id=(q, c), device_id_type=MESH,
        )

    @pl.when(r == 0)
    def _():
        for q in range(1, nr):
            scatter(q).start()

    pltpu.make_async_copy(raw, raw, raw_sem).wait()
    for k in range(COLS):
        for m in range(subs):
            mine[k, m : m + 1, :] = raw[k : k + 1, m * LANES : (m + 1) * LANES]
    spot = c * nr + r
    panel[spot] = mine[...]

    def spread(d, carry):
        t = lax.rem(here + d, n)
        pltpu.make_async_remote_copy(
            src_ref=mine, dst_ref=panel.at[spot], send_sem=psend_sem, recv_sem=precv_sem,
            device_id=(t // nc, lax.rem(t, nc)), device_id_type=MESH,
        ).start()
        return carry

    lax.fori_loop(1, n, spread, 0)
    most = panel.at[pl.ds(0, n - 1)]
    pltpu.make_async_copy(most, most, precv_sem).wait()
    pltpu.make_async_copy(most, most, psend_sem).wait()

    @pl.when(r == 0)
    def _():
        for q in range(1, nr):
            scatter(q).wait_send()

    ids = lax.broadcasted_iota(jnp.int32, (subs, LANES), 0) * LANES + lax.broadcasted_iota(
        jnp.int32, (subs, LANES), 1
    )

    def reflect(column, current):
        vecs[column] = current
        head = jnp.where(ids > column, current[0], 0.0)
        vecs[column, 0] = head
        below = vecs[column]
        squared = total(below * below)
        leading = pick(head, ids == column + 1)
        length = jnp.sqrt(squared)
        vecs[column, 0] = head + jnp.where(ids == column + 1, length, 0.0)
        return 1.0 / (length * (length + leading))

    def step(j, scaling):
        vrows = [
            jnp.broadcast_to(vecs[j, c * nr + t // subs, t % subs : t % subs + 1, :], (8, LANES))
            for t in range(tiles)
        ]

        def block(i, carry):
            k = turn(i)

            @pl.when(j == 0)
            def _():
                load(i).wait()

            def group(g, inner):
                at = pl.ds(pl.multiple_of(k * quarter + g * 8, 8), 8)
                sums = [None] * 4
                for t in range(tiles):
                    term = a[at, t * LANES : (t + 1) * LANES] * vrows[t]
                    sums[t % 4] = term if sums[t % 4] is None else sums[t % 4] + term
                acc[pl.ds(pl.multiple_of(g * 8, 8), 8), :] = (sums[0] + sums[1]) + (sums[2] + sums[3])
                return inner

            lax.fori_loop(0, quarter // 8, group, 0, unroll=16)
            for m in range(subs):
                turned = acc[m * LANES : (m + 1) * LANES, :].T
                part[k, m : m + 1, :] = jnp.sum(turned, axis=0, keepdims=True)

            @pl.when(i < nc - 1)
            def _():
                first(k).start()

            return carry

        def first(k):
            return pltpu.make_async_remote_copy(
                src_ref=part.at[k], dst_ref=arrived.at[c], send_sem=send1_sem.at[k],
                recv_sem=recv1_sem.at[c], device_id=(r, k), device_id_type=MESH,
            )

        lax.fori_loop(0, nc, block, 0)
        value = part[c]

        def collect(d, value):
            k = lax.rem(c + d, nc)
            pltpu.make_async_copy(arrived.at[k], arrived.at[k], recv1_sem.at[k]).wait()
            return value + arrived[k]

        value = lax.fori_loop(1, nc, collect, value, unroll=True)
        image[j, here] = value

        def second(d, carry):
            t = lax.rem(here + d, n)
            pltpu.make_async_remote_copy(
                src_ref=image.at[j, here], dst_ref=image.at[j, here], send_sem=send2_sem,
                recv_sem=recv2_sem.at[j], device_id=(t // nc, lax.rem(t, nc)), device_id_type=MESH,
            ).start()
            return carry

        for d in sorted(range(1, n), key=lambda d: abs(d - n // 2)):
            second(d, 0)

        vector = vecs[j]
        corr[...] = jnp.zeros(corr.shape, jnp.float32)
        follow = jnp.minimum(j + 1, COLS - 1)
        nxt[...] = panel[:, follow]
        target = ids == j + 1

        def history(k, carry):
            v_k = vecs[k]
            w_k = comps[k]
            corr[...] = corr[...] + v_k * total(w_k * vecs[j]) + w_k * total(v_k * vecs[j])
            nxt[...] = nxt[...] - v_k * pick(w_k[0], target) - w_k * pick(v_k[0], target)
            return carry

        lax.fori_loop(0, j, history, 0)

        def sent(d, carry):
            k = lax.rem(c + d, nc)
            pltpu.make_async_copy(part.at[k], part.at[k], send1_sem.at[k]).wait()
            return carry

        lax.fori_loop(1, nc, sent, 0)
        rest = image.at[j, pl.ds(0, n - 1)]
        pltpu.make_async_copy(rest, rest, send2_sem).wait()
        pltpu.make_async_copy(rest, rest, recv2_sem.at[j]).wait()

        pushed = scaling * (image[j] - corr[...])
        inner_product = total(pushed * vector)
        update = pushed - (0.5 * scaling * inner_product) * vector
        comps[j] = update
        current = nxt[...] - vector * pick(update[0], target) - update * pick(vector[0], target)
        return reflect(j + 1, current)

    lax.fori_loop(0, COLS, step, reflect(0, panel[:, 0]))

    def place(dest, base, count):
        def move(p, carry):
            for m in range(subs):
                at = pl.ds(pl.multiple_of((p * subs + m) * LANES, LANES), LANES)
                for k in range(COLS):
                    dest[k : k + 1, at] = vecs[k, base + p, m : m + 1, :]
                    dest[COLS + k : COLS + k + 1, at] = comps[k, base + p, m : m + 1, :]
            return carry

        lax.fori_loop(0, count, move, 0)

    place(left_ref, r * nc, nc)
    place(right_ref, c * nr, nr)
    left_ref[2 * COLS :, :] = jnp.zeros((COLS, rows), jnp.float32)


def plain_call(nr, nc, matrix):
    rows, cols = matrix.shape
    n = nr * nc
    subs = rows // nc // LANES
    vector = (n, subs, LANES)
    f32 = jnp.float32
    vmem = pl.BlockSpec(memory_space=pltpu.VMEM)
    dma = pltpu.SemaphoreType.DMA
    return pl.pallas_call(
        functools.partial(plain_kernel, nr, nc),
        out_shape=(
            jax.ShapeDtypeStruct((3 * COLS, rows), f32),
            jax.ShapeDtypeStruct((2 * COLS, cols), f32),
            pltpu.VMEM((rows, cols), f32),
        ),
        in_specs=[pl.BlockSpec(memory_space=pl.ANY)],
        out_specs=(vmem, vmem, vmem),
        scratch_shapes=[
            pltpu.VMEM((COLS, cols // nr), f32),
            pltpu.VMEM((COLS, subs, LANES), f32),
            pltpu.VMEM((n, COLS, subs, LANES), f32),
            pltpu.VMEM((rows // nc, LANES), f32),
            pltpu.VMEM((nc, subs, LANES), f32),
            pltpu.VMEM((nc, subs, LANES), f32),
            pltpu.VMEM((COLS,) + vector, f32),
            pltpu.VMEM((COLS + 1,) + vector, f32),
            pltpu.VMEM((COLS + 1,) + vector, f32),
            pltpu.VMEM(vector, f32),
            pltpu.VMEM(vector, f32),
            dma((nc,)), dma((nr,)), dma, dma, dma,
            dma((nc,)), dma((nc,)), dma, dma((COLS,)),
        ],
        compiler_params=pltpu.CompilerParams(
            collective_id=1, has_side_effects=True, vmem_limit_bytes=8 * 1024 * 1024
        ),
    )(matrix)


def lane_sum(values):
    return jnp.broadcast_to(jnp.sum(values, axis=1, keepdims=True), values.shape)


def row_sum(values):
    return jnp.sum(values, axis=0, keepdims=True)


def panel_kernel(
    nr, nc, a_hbm, left_ref, right_ref, a,
    lanes, acc, pan_r, pan_c, pan_h, head_out,
    v_r, w_r, y_r, m_r, p_r, q_r, z_r, base_r,
    v_c, w_c, y_c, m_c, p_c, q_c, z_c, base_c,
    v_h, w_h, g_old, h_old, g_new, h_new, wj_next, vj_next, keep, dots,
    part_c, part_r, note_r, note_c,
    load_sem, strip_sem, pan_send, pan_recv, cross_send, pan_cross, rest_send, pan_rest, head_send, head_recv,
    part_send, part_recv, back_send, back_recv, far_send, far_recv,
    rows_send, rows_recv, note_send, note_r_recv, note_c_recv,
):
    r = lax.axis_index("row")
    c = lax.axis_index("col")
    n = nr * nc
    here = r * nc + c
    rows, cols = a.shape
    deep = rows // LANES
    wide = cols // LANES
    chunks = wide // 8
    width = cols // chunks
    half = deep // 2
    group = nr // (nc // 2)
    side = lax.rem(c, 2)
    owner = r // 2
    f32 = jnp.float32

    def load(q):
        return pltpu.make_async_copy(
            a_hbm.at[:, pl.ds(q * width, width)], a.at[:, pl.ds(q * width, width)], load_sem.at[q]
        )

    strip = pltpu.make_async_copy(a_hbm.at[:, pl.ds(0, LANES)], lanes, strip_sem)

    @pl.when(c == 0)
    def _():
        strip.start()

    @pl.when(c != 0)
    def _():
        for q in range(chunks):
            load(q).start()

    barrier = pltpu.get_barrier_semaphore()

    def greet(d, carry):
        t = lax.rem(here + d, n)
        pl.semaphore_signal(barrier, inc=1, device_id=(t // nc, lax.rem(t, nc)), device_id_type=MESH)
        return carry

    lax.fori_loop(1, n, greet, 0)

    for ref in (v_r, w_r, v_c, w_c, v_h, w_h, g_old, h_old, keep, dots, p_r, p_c):
        ref[...] = jnp.zeros(ref.shape, f32)
    y_r[0] = jnp.zeros(y_r.shape[1:], f32)
    y_c[0] = jnp.zeros(y_c.shape[1:], f32)

    def to(src, dst, send, recv, row, col):
        return pltpu.make_async_remote_copy(
            src_ref=src, dst_ref=dst, send_sem=send, recv_sem=recv,
            device_id=(row, col), device_id_type=MESH,
        )

    def drain(ref, sem):
        pltpu.make_async_copy(ref, ref, sem).wait()

    used = pl.ds(0, COLS + 1)
    first = pl.ds(0, 2)
    others = pl.ds(2, COLS - 1)

    @pl.when(c == 0)
    def _():
        strip.wait()
        for q in range(chunks):
            load(q).start()

        def turn(b, carry):
            turned = lanes[pl.ds(pl.multiple_of(b * LANES, LANES), LANES), :].T
            for k in range(COLS + 1):
                pan_r[k, pl.ds(b, 1), :] = turned[k : k + 1, :]
            return carry

        lax.fori_loop(0, deep, turn, 0)

    pl.semaphore_wait(barrier, n - 1)

    @pl.when(c == 0)
    def _():
        for d in range(1, nc):
            to(pan_r.at[first], pan_r.at[first], pan_send.at[d - 1], pan_recv.at[0], r, d).start()
        for d in range(1, nc):
            to(pan_r.at[others], pan_r.at[others], pan_send.at[nc + d - 1], pan_recv.at[1], r, d).start()

    @pl.when(c != 0)
    def _():
        drain(pan_r.at[first], pan_recv.at[0])

    def spread(source, target, width_of, send, recv):
        for i in range(group):
            row = (c // 2) * group + i
            mine = jnp.logical_and(row == r, c == owner)

            @pl.when(jnp.logical_not(mine))
            def _(i=i, row=row):
                to(source(side), target(lax.rem(r, 2), side), send.at[i], recv.at[2 * lax.rem(r, 2) + side], row, owner).start()

    def collect(target, recv):
        for kind in range(2):
            for part in range(2):
                mine = jnp.logical_and(r == 2 * c + kind, c == part + 2 * (r // group))

                @pl.when(jnp.logical_not(mine))
                def _(kind=kind, part=part):
                    drain(target(kind, part), recv.at[2 * kind + part])

    def spread_done(source, send):
        for i in range(group):
            row = (c // 2) * group + i
            mine = jnp.logical_and(row == r, c == owner)

            @pl.when(jnp.logical_not(mine))
            def _(i=i):
                drain(source(side), send.at[i])

    def keeps_own():
        return jnp.logical_and(c == owner, r // group == c // 2)

    def piece(part):
        return pl.ds(pl.multiple_of(part * half, half), half)

    def spot(kind, part):
        return pl.ds(pl.multiple_of(kind * deep + part * half, half), half)

    def share_panel(part_of, send, recv):
        spread(lambda part: pan_r.at[part_of, piece(part)], lambda kind, part: pan_c.at[part_of, spot(kind, part)], None, send, recv)

        @pl.when(keeps_own())
        def _():
            pan_c[part_of, spot(lax.rem(r, 2), side)] = pan_r[part_of, piece(side)]

    def take_panel(part_of, recv):
        collect(lambda kind, part: pan_c.at[part_of, spot(kind, part)], recv)

    def share_head():
        @pl.when(c != 0)
        def _():
            drain(pan_r.at[others], pan_recv.at[1])

        @pl.when(r == 0)
        def _():
            for k in range(COLS + 1):
                head_out[k : k + 1, :] = pan_r[k, 0:1, :]
                pan_h[k : k + 1, :] = pan_r[k, 0:1, :]
            for d in range(1, nr):
                to(head_out, pan_h, head_send.at[d - 1], head_recv, d, c).start()

    share_panel(first, cross_send, pan_cross)

    ids_r = (
        r * rows
        + lax.broadcasted_iota(jnp.int32, (deep, LANES), 0) * LANES
        + lax.broadcasted_iota(jnp.int32, (deep, LANES), 1)
    )
    ids_c = (
        c * cols
        + lax.broadcasted_iota(jnp.int32, (wide, LANES), 0) * LANES
        + lax.broadcasted_iota(jnp.int32, (wide, LANES), 1)
    )
    lane1 = lax.broadcasted_iota(jnp.int32, (1, LANES), 1)
    lane8 = lax.broadcasted_iota(jnp.int32, (8, LANES), 1)
    row8 = lax.broadcasted_iota(jnp.int32, (8, LANES), 0)
    lane24 = lax.broadcasted_iota(jnp.int32, (24, LANES), 1)
    row24 = lax.broadcasted_iota(jnp.int32, (24, LANES), 0)

    dom_r = (pan_r, v_r, w_r, y_r, m_r, p_r, q_r, z_r, base_r, ids_r)
    dom_c = (pan_c, v_c, w_c, y_c, m_c, p_c, q_c, z_c, base_c, ids_c)

    m_r[...] = jnp.where(ids_r > 0, pan_r[0], 0.0)

    def send_notes(j, dom, note, slot, me, count, peer):
        _, v, w, y, m, p, _, _, _, ids = dom
        jm = jnp.maximum(j - 1, 0)
        operand = m[...]
        push = p[...]
        last = v[jm]
        for k in range(COLS):
            dots[k : k + 1, :] = row_sum(w[k] * operand)
            dots[COLS + k : COLS + k + 1, :] = row_sum(v[k] * operand)
        cut = jnp.where(ids > j, last, 0.0)
        dots[16:17, :] = row_sum(push * operand)
        dots[17:18, :] = row_sum(push * last)
        dots[18:19, :] = row_sum(operand * operand)
        dots[19:20, :] = row_sum(operand * cut)
        dots[20:21, :] = row_sum(cut * cut)
        sums = lane_sum(dots[...])
        note[slot, me, 0:1, :] = row_sum(jnp.where(lane24 == row24, sums, 0.0))
        note[slot, me, 1:2, :] = y[j, 0:1, :]
        recv = note_r_recv if count == nr else note_c_recv
        for d in range(1, count):
            row, col = peer(d)
            to(note.at[slot, me], note.at[slot, me], note_send, recv.at[slot], row, col).start()

    def take_notes(note, slot, count):
        recv = note_r_recv if count == nr else note_c_recv
        drain(note.at[slot, pl.ds(0, count - 1)], recv.at[slot])
        drain(note.at[slot, pl.ds(0, count - 1)], note_send)
        total = note[slot, 0, 0:1, :]
        for k in range(1, count):
            total = total + note[slot, k, 0:1, :]
        spread24 = jnp.broadcast_to(total, (24, LANES))
        return lane_sum(jnp.where(lane24 == row24, spread24, 0.0)), note[slot, 0, 1:2, :]

    def settle(j, dom, out, sums, y_head):
        jm = jnp.maximum(j - 1, 0)
        jrow = pl.ds(jm, 1)
        s_old = keep[0:1, :]
        bad = keep[1:2, :]
        pm, pv, mm, mv, vv = (sums[16 + i : 17 + i, :] for i in range(5))
        alpha = 0.5 * s_old * pv
        gold = g_old[...]
        hold = h_old[...]
        vh = v_h[...]
        pan, v, w, y, m, p, _, _, _, ids = out
        old = y[j]
        s1 = jnp.zeros(old.shape, f32)
        for k in range(COLS):
            s1 = s1 + v[k] * gold[k : k + 1, :] + w[k] * hold[k : k + 1, :]
        p_head = s_old * (y_head - row_sum(vh * gold + w_h[...] * hold))
        v_head = v_h[jrow, :]
        w_h[jrow, :] = p_head - alpha * v_head
        wh = w_h[...]
        now8 = lane8 == j
        next8 = lane8 == j + 1
        vj = lane_sum(jnp.where(now8, vh, 0.0))
        wj = lane_sum(jnp.where(now8, wh, 0.0))
        vn = lane_sum(jnp.where(next8, vh, 0.0))
        wn = lane_sum(jnp.where(next8, wh, 0.0))
        v_at = lane_sum(jnp.where(lane1 == j, v_head, 0.0))
        p_at = lane_sum(jnp.where(lane1 == j, p_head, 0.0))
        coef = 2.0 * alpha * v_at - p_at
        before = row8 < j - 1
        vjb = jnp.where(before, vj, 0.0)
        wjb = jnp.where(before, wj, 0.0)
        x_head = pan_h[pl.ds(j, 1), :] - row_sum(vh * wjb + wh * vjb) - p_head * v_at
        b_head = jnp.where(lane1 > j, x_head + coef * v_head, 0.0)
        lead = lane_sum(jnp.where(lane1 == j + 1, b_head, 0.0))
        squared = mm + 2.0 * coef * mv + coef * coef * vv
        length = jnp.sqrt(squared)
        v_h[pl.ds(j, 1), :] = b_head + jnp.where(lane1 == j + 1, length, 0.0)
        scale = 1.0 / (length * (length + lead))
        pivot = lead + length
        kappa = scale * pivot
        fine = (mm + coef * coef * vv) <= GUARD * squared
        keep[0:1, :] = scale
        keep[1:2, :] = jnp.where(fine, bad, 1.0)
        keep[2:3, :] = kappa
        at_last = row8 == jm
        v_sq = vv + v_at * v_at
        gold = gold + jnp.where(at_last, pv - alpha * v_sq, 0.0)
        hold = hold + jnp.where(at_last, v_sq, 0.0)
        gn = sums[0:8, :] + jnp.where(at_last, pm - alpha * mv, 0.0) + coef * (gold - wj * v_at) + length * wn
        hn = sums[8:16, :] + coef * (hold - vj * v_at) + length * vn
        live = row8 < j
        gn = jnp.where(live, gn, 0.0)
        hn = jnp.where(live, hn, 0.0)
        g_old[...] = gn
        h_old[...] = hn

        _, vd, wd, _, md, pd, _, _, _, ids_d = dom
        last_d = vd[jm]
        wd[jm] = pd[...] - alpha * last_d
        vd[j] = (
            md[...] + coef * jnp.where(ids_d > j, last_d, 0.0) + jnp.where(ids_d == j + 1, length, 0.0)
        )

        last = v[jm]
        push = s_old * (old - s1)
        w[jm] = push - alpha * last
        s2 = jnp.zeros(old.shape, f32)
        s3 = jnp.zeros(old.shape, f32)
        s4 = jnp.zeros(old.shape, f32)
        for k in range(COLS):
            v_k = v[k]
            w_k = w[k]
            s2 = s2 + v_k * wjb[k : k + 1, :] + w_k * vjb[k : k + 1, :]
            s3 = s3 + v_k * gn[k : k + 1, :] + w_k * hn[k : k + 1, :]
            s4 = s4 + v_k * wn[k : k + 1, :] + w_k * vn[k : k + 1, :]
        a_now = pan[j]
        a_next = pan[j + 1]
        x = a_now - s2 - push * v_at
        b = jnp.where(ids > j, x + coef * last, 0.0)
        v[j] = b + jnp.where(ids == j + 1, length, 0.0)
        extra = coef * (old - v_at * a_now) + length * a_next
        out[6][...] = extra
        base = extra - s3
        out[8][...] = base
        out[7][...] = a_next - s4 - kappa * base

    def absorb(j, out, at, value):
        _, _, _, y, m, p, extra, z, base, ids = out
        scale = keep[0:1, :]
        kappa = keep[2:3, :]
        y[j + 1, at, :] = value + extra[at, :]
        p[at, :] = scale * (value + base[at, :])
        return z[at, :] - kappa * value

    blocks = rows // LANES
    batch = 4
    groups = LANES // 8

    def tile(row, t):
        return a[pl.ds(pl.multiple_of(row, 8), 8), t * LANES : (t + 1) * LANES]

    def turn_rows(b):
        for k in range(batch):
            at = pl.ds(pl.multiple_of((b * batch + k) * LANES, LANES), LANES)
            lanes[at, :] = jnp.broadcast_to(m_r[pl.ds(b * batch + k, 1), :], (LANES, LANES)).T

    def down(q):
        many = batch if q == 0 else 1

        def block(b, sums):
            factors = [
                lanes[pl.ds(pl.multiple_of(b * many * LANES + g * 8, 8), 8), :]
                for g in range(many * groups)
            ]
            if q == 0:
                turn_rows(jnp.minimum(b + 1, blocks // batch - 1))
            for g in range(many * groups):
                row = b * many * LANES + g * 8
                sums = tuple(
                    sums[t] + tile(row, q * 8 + t) * factors[g] for t in range(8)
                )
            return sums

        if q == 0:
            turn_rows(0)
        return lax.fori_loop(0, blocks // many, block, tuple(jnp.zeros((8, LANES), f32) for _ in range(8)))

    def across(q, slot):
        factors = [jnp.broadcast_to(m_c[q * 8 + t : q * 8 + t + 1, :], (8, LANES)) for t in range(8)]
        final = q == chunks - 1
        many = batch if final else 1

        def fold(b):
            for k in range(batch):
                turned = acc[pl.ds(pl.multiple_of((b * batch + k) * LANES, LANES), LANES), :].T
                part_r[slot, c, pl.ds(b * batch + k, 1), :] = row_sum(turned)

        def block(b, carry):
            if final:
                fold(jnp.maximum(b - 1, 0))
            for g in range(many * groups):
                row = b * many * LANES + g * 8
                at = pl.ds(pl.multiple_of(row, 8), 8)
                terms = [tile(row, q * 8 + t) * factors[t] for t in range(8)]
                while len(terms) > 1:
                    terms = [terms[i] + terms[i + 1] for i in range(0, len(terms), 2)]
                acc[at, :] = terms[0] if q == 0 else acc[at, :] + terms[0]
            return carry

        lax.fori_loop(0, blocks // many, block, 0)
        if final:
            fold(blocks // batch - 1)

    def in_rows(d):
        return lax.rem(r + d, nr), c

    def in_cols(d):
        return r, lax.rem(c + d, nc)

    def back_source(j):
        return y_c.at[j + 1, pl.ds(pl.multiple_of(lax.rem(r, 2) * deep, deep), deep)]

    def pair(i, carry):
        j = 2 * i
        send_notes(j, dom_r, note_r, i, r, nr, in_rows)
        for q in range(chunks):
            @pl.when(i == 0)
            def _(q=q):
                load(q).wait()
                if q == 1:
                    share_head()

            sums = down(q)
            for t in range(8):
                part_c[i, q, r, t : t + 1, :] = row_sum(sums[t])
            for d in sorted(range(1, nr), key=lambda d: abs(d - nr // 2)):
                row, col = in_rows(d)
                mine = part_c.at[i, q, r]
                to(mine, mine, part_send, part_recv.at[i, q], row, col).start()

        @pl.when(i == 0)
        def _():
            share_panel(others, rest_send, pan_rest)
            take_panel(first, pan_cross)

            @pl.when(r != 0)
            def _():
                drain(pan_h, head_recv)

        @pl.when(i > 0)
        def _():
            collect(lambda kind, part: y_c.at[j, spot(kind, part)], far_recv.at[i])
            spread_done(lambda part: y_r.at[j, piece(part)], far_send)
            drain(part_r.at[i, pl.ds(0, nc - 1)], rows_send)

        @pl.when(i == 1)
        def _():
            take_panel(others, pan_rest)

        sums, y_head = take_notes(note_r, i, nr)
        settle(j, dom_r, dom_c, sums, y_head)

        for q in range(chunks):
            drain(part_c.at[i, q, pl.ds(0, nr - 1)], part_recv.at[i, q])
            value = part_c[i, q, 0]
            for k in range(1, nr):
                value = value + part_c[i, q, k]
            at = pl.ds(q * 8, 8)
            m_c[at, :] = jnp.where(ids_c[q * 8 : q * 8 + 8, :] > j + 1, absorb(j, dom_c, at, value), 0.0)
            if q == chunks - 1:
                @pl.when(c == owner)
                def _():
                    for d in range(1, nc):
                        to(back_source(j), y_r.at[j + 1], back_send.at[d - 1], back_recv.at[i], r, lax.rem(c + d, nc)).start()
                    y_r[j + 1] = y_c[j + 1, pl.ds(pl.multiple_of(lax.rem(r, 2) * deep, deep), deep)]

                send_notes(j + 1, dom_c, note_c, i, c, nc, in_cols)
            across(q, i)

        mine = part_r.at[i, c]
        for d in range(1, nc):
            row, col = in_cols(d)
            to(mine, mine, rows_send, rows_recv.at[i], row, col).start()
        drain(part_c.at[i, :, pl.ds(0, nr - 1)], part_send)

        @pl.when(c != owner)
        def _():
            drain(y_r.at[j + 1], back_recv.at[i])

        @pl.when(c == owner)
        def _():
            for d in range(1, nc):
                drain(back_source(j), back_send.at[d - 1])

        sums, y_head = take_notes(note_c, i, nc)
        settle(j + 1, dom_c, dom_r, sums, y_head)
        drain(part_r.at[i, pl.ds(0, nc - 1)], rows_recv.at[i])
        value = part_r[i, 0]
        for k in range(1, nc):
            value = value + part_r[i, k]
        m_r[...] = jnp.where(ids_r > j + 2, absorb(j + 1, dom_r, slice(None), value), 0.0)

        def far_source(part):
            return y_r.at[j + 2, piece(part)]

        spread(far_source, lambda kind, part: y_c.at[j + 2, spot(kind, part)], None, far_send, far_recv.at[i + 1])

        @pl.when(keeps_own())
        def _():
            y_c[j + 2, spot(lax.rem(r, 2), side)] = y_r[j + 2, piece(side)]

        return carry

    lax.fori_loop(0, COLS // 2, pair, 0)

    last = COLS // 2
    send_notes(COLS, dom_r, note_r, last, r, nr, in_rows)

    @pl.when(c == 0)
    def _():
        for d in range(1, nc):
            drain(pan_r.at[first], pan_send.at[d - 1])
            drain(pan_r.at[others], pan_send.at[nc + d - 1])

    spread_done(lambda part: pan_r.at[first, piece(part)], cross_send)
    spread_done(lambda part: pan_r.at[others, piece(part)], rest_send)

    @pl.when(r == 0)
    def _():
        for d in range(1, nr):
            drain(head_out, head_send.at[d - 1])

    def place(dest, values, base, blocks_of):
        for b in range(blocks_of):
            for k in range(COLS):
                dest[base + k : base + k + 1, b * LANES : (b + 1) * LANES] = values[k, b : b + 1, :]

    place(left_ref, v_r, 0, deep)
    place(right_ref, v_c, 0, wide)
    collect(lambda kind, part: y_c.at[COLS, spot(kind, part)], far_recv.at[last])
    spread_done(lambda part: y_r.at[COLS, piece(part)], far_send)
    drain(part_r.at[0, pl.ds(0, nc - 1)], rows_send)
    sums, _ = take_notes(note_r, last, nr)
    scale = keep[0:1, :]
    alpha = 0.5 * scale * sums[17:18, :]
    w_r[COLS - 1] = p_r[...] - alpha * v_r[COLS - 1]
    s1 = jnp.zeros((wide, LANES), f32)
    for k in range(COLS - 1):
        s1 = s1 + v_c[k] * g_old[k : k + 1, :] + w_c[k] * h_old[k : k + 1, :]
    w_c[COLS - 1] = scale * (y_c[COLS] - s1) - alpha * v_c[COLS - 1]
    place(left_ref, w_r, COLS, deep)
    place(right_ref, w_c, COLS, wide)
    left_ref[2 * COLS :, :] = jnp.broadcast_to(keep[1:2, 0:1], (COLS, rows))


def panel_call(nr, nc, matrix):
    rows, cols = matrix.shape
    deep, wide = rows // LANES, cols // LANES
    chunks = wide // 8
    f32 = jnp.float32
    vmem = pl.BlockSpec(memory_space=pltpu.VMEM)
    dma = pltpu.SemaphoreType.DMA
    steps = COLS // 2

    def mem(*shape):
        return pltpu.VMEM(shape, f32)

    def domain(size):
        return [
            mem(COLS + 1, size, LANES), mem(COLS + 1, size, LANES), mem(COLS + 1, size, LANES),
            *(mem(size, LANES) for _ in range(5)),
        ]

    return pl.pallas_call(
        functools.partial(panel_kernel, nr, nc),
        out_shape=(
            jax.ShapeDtypeStruct((3 * COLS, rows), f32),
            jax.ShapeDtypeStruct((2 * COLS, cols), f32),
            pltpu.VMEM((rows, cols), f32),
        ),
        in_specs=[pl.BlockSpec(memory_space=pl.ANY)],
        out_specs=(vmem, vmem, vmem),
        scratch_shapes=[
            mem(rows, LANES), mem(rows, LANES),
            mem(COLS + 1, deep, LANES), mem(COLS + 1, wide, LANES), mem(16, LANES), mem(16, LANES),
            *domain(deep), *domain(wide),
            mem(8, LANES), mem(8, LANES), mem(8, LANES), mem(8, LANES), mem(8, LANES), mem(8, LANES),
            mem(8, LANES), mem(8, LANES), mem(8, LANES), mem(24, LANES),
            mem(steps, chunks, nr, 8, LANES), mem(steps, nc, deep, LANES),
            mem(steps + 1, nr, 2, LANES), mem(steps, nc, 2, LANES),
            dma((chunks,)), dma, dma((2 * nc,)), dma((2,)), dma((nr,)), dma((4,)), dma((nr,)), dma((4,)), dma((nr,)), dma,
            dma, dma((steps, chunks)), dma((nc,)), dma((steps,)), dma((nr,)), dma((steps + 1, 4)),
            dma, dma((steps,)), dma, dma((steps + 1,)), dma((steps,)),
        ],
        compiler_params=pltpu.CompilerParams(
            collective_id=0, has_side_effects=True, vmem_limit_bytes=8 * 1024 * 1024
        ),
    )(matrix)


def thirds(values):
    high = values.astype(jnp.bfloat16)
    rest = values - high.astype(jnp.float32)
    middle = rest.astype(jnp.bfloat16)
    low = (rest - middle.astype(jnp.float32)).astype(jnp.bfloat16)
    return high, middle, low


SLOTS = 4


def trailing_kernel(left_ref, right_ref, a_ref, out_ref, refl_ref, flag_ref, stacked, stage, sem):
    slots, tile, _ = stage.shape
    steps = a_ref.shape[0] // tile
    swapped = jnp.concatenate([right_ref[COLS:, :], right_ref[:COLS, :]], axis=0)
    h, m, l = thirds(swapped)
    stacked[...] = jnp.concatenate([h, m, h, m, l, h], axis=0)

    def copy(step, slot):
        at = pl.ds(pl.multiple_of(step * tile, tile), tile)
        return pltpu.make_async_copy(stage.at[slot], out_ref.at[at], sem.at[slot])

    def run(step, carry):
        slot = lax.rem(step, slots)

        @pl.when(step >= slots)
        def _():
            copy(step - slots, slot).wait()

        at = pl.ds(pl.multiple_of(step * tile, tile), tile)
        h, m, l = thirds(left_ref[: 2 * COLS, at])
        other = jnp.concatenate([h, h, m, m, h, l], axis=0)
        product = lax.dot_general(
            other, stacked[...], (((0,), (0,)), ((), ())), preferred_element_type=jnp.float32
        )
        stage[slot] = a_ref[at, :] - product
        copy(step, slot).start()
        return carry

    lax.fori_loop(0, steps, run, 0)
    refl_ref[...] = left_ref[:COLS, :]
    flag_ref[...] = left_ref[2 * COLS :, :LANES]
    for k in range(slots):
        step = steps - slots + k
        copy(step, step % slots).wait()


def trailing_call(left, right, matrix):
    rows, cols = matrix.shape
    tile = 128
    vmem = pl.BlockSpec(memory_space=pltpu.VMEM)
    return pl.pallas_call(
        trailing_kernel,
        out_shape=(
            jax.ShapeDtypeStruct((rows, cols), jnp.float32),
            jax.ShapeDtypeStruct((COLS, rows), jnp.float32),
            jax.ShapeDtypeStruct((COLS, LANES), jnp.float32),
        ),
        in_specs=[vmem, vmem, vmem],
        out_specs=(pl.BlockSpec(memory_space=pl.ANY), vmem, vmem),
        scratch_shapes=[
            pltpu.VMEM((12 * COLS, cols), jnp.bfloat16),
            pltpu.VMEM((min(SLOTS, rows // tile), tile, cols), jnp.float32),
            pltpu.SemaphoreType.DMA((min(SLOTS, rows // tile),)),
        ],
        compiler_params=pltpu.CompilerParams(vmem_limit_bytes=16 * 1024 * 1024),
    )(left, right, matrix)


def local(nr, nc, matrix):
    rows, cols = matrix.shape
    piece = rows // nc
    if rows % (16 * LANES) or cols != 2 * rows or nr != 2 * nc or nc % 2 or piece > 8 * LANES:
        return local_general(matrix)
    left, right, kept = panel_call(nr, nc, matrix)
    trailing, reflectors, flag = trailing_call(left, right, kept)

    def again(state):
        own, _ = lax.optimization_barrier((matrix, state[2]))
        return trailing_call(*plain_call(nr, nc, own))

    trailing, reflectors, _ = lax.while_loop(
        lambda state: jnp.any(state[2] != 0.0), again, (trailing, reflectors, flag)
    )
    return trailing, reflectors.T


def solution(mesh):
    return jax.shard_map(
        functools.partial(local, mesh.shape["row"], mesh.shape["col"]),
        mesh=mesh,
        in_specs=(P("row", "col"),),
        out_specs=(P("row", "col"), P("row", None)),
        check_vma=False,
    )
```
